32 devices in a mesh: row: 4 (over z), col: 8 (over y, x, core).
Axes of the slice: x: 2, y: 2, z: 4, core: 2. Of those that a mesh axis runs over, the one named last changes fastest.
Arguments:
- working: float32 [16, 4, 256, 8, 8, 256], P(None, 'row', None, None, 'col'), may hold values from -6 to 6
- factor_panel: float32 [2, 16, 4, 256, 256], P(None, None, 'row'), may hold values from -0.12 to 2, as said below
Outputs:
- gram_part: float32 [16, 4, 256, 8, 8, 256], P(None, 'row', None, None, 'col')
- finished_columns: float32 [8, 4, 256, 8, 4, 512], P(None, None, None, 'col', 'row')
The draws below stay inside these ranges and needn't reach their ends.
Inputs may be any that keep to these rules, and one draw needn't show every extreme that they name: factor_panel holds a lower-triangular factor: entries above the factor's diagonal are zero and its diagonal entries lie between 1 and 2.
All inputs are finite; a program needn't handle non-finite values.
Results may differ from the reference program's by a relative error of at most 0.0001.
Values sent between devices are 32-bit elements; how exact they have to be, the bound alone decides.
No kernel may reach another device: no remote copies, remote signals or barrier semaphores. Data moves between devices by JAX's collectives and lax.ppermute only.
A program may use at most 256 MiB of HBM per device.

```python
import jax
import jax.numpy as jnp
from jax import lax

N = 16384
BLK = 256
K = 30
STEPS = 2
FIN = 32
LR = 16
LC = 8
LF = 8
CW = 512
N_ROW = 4
N_COL = 8


def draw_factor_panel(key, part):
    keys = jax.random.split(jax.random.fold_in(key, 17), 2)
    below = jnp.clip(jax.random.normal(keys[0], (STEPS, N, BLK), jnp.float32) * 0.03, -0.12, 0.12)
    diagonal_values = jax.random.uniform(keys[1], (STEPS, 1, BLK), jnp.float32, 1.0, 2.0)
    row_block = (jnp.arange(N) // BLK)[None, :, None]
    within = (jnp.arange(N) % BLK)[None, :, None]
    column = jnp.arange(BLK)[None, None, :]
    target = (K + jnp.arange(STEPS))[:, None, None]
    inside = jnp.where(within > column, 0.5 * below, jnp.where(within == column, diagonal_values, 0.0))
    values = jnp.where(row_block > target, below, jnp.where(row_block == target, inside, 0.0))
    return values.reshape(STEPS, LR, N // (LR * BLK), BLK, BLK)


def block_scale(stream_key, shape, cuts, smallest, top_value):
    def one(position, blocks):
        draws = jax.random.uniform(jax.random.fold_in(jax.random.fold_in(stream_key, 6), position), (blocks,), jnp.float32, smallest / len(cuts), top_value / len(cuts))
        return jnp.repeat(jnp.exp(draws), shape[position] // blocks).reshape((-1,) + (1,) * (len(shape) - position - 1))

    gain = one(*cuts[0])
    for cut in cuts[1:]:
        gain = gain * one(*cut)
    return gain


def centred(rng, extent, spread, limit, cuts=(), held_as=jnp.bfloat16):
    drawn = jax.random.normal(rng, extent, jnp.float32) * spread
    if len(cuts) > 0:
        drawn = block_scale(rng, extent, cuts, -0.22, 0.18) * drawn
    return jnp.clip(drawn, min=-limit, max=limit).astype(held_as)


def setup_inputs(seed: int = 0) -> dict:
    streams_of = jax.random.split(jax.random.key(seed), 3)
    return {
        "working": centred(streams_of[0], (LR, N_ROW, BLK, LC, N_COL, BLK), 1.0, 6.0, ((1, 4), (4, 8)), jnp.float32),
        "factor_panel": draw_factor_panel(jax.random.fold_in(streams_of[2], 71), 0),
    }


def reference(working, factor_panel):
    matrix = working.reshape(N, N)
    row_block = jnp.arange(N) // BLK
    solved_list = []
    for step_index in range(STEPS):
        target = K + step_index
        column = factor_panel[step_index].reshape(N, BLK)
        diagonal = jnp.tril(column[target * BLK:(target + 1) * BLK])
        solved = lax.linalg.triangular_solve(diagonal, matrix[target * BLK:(target + 1) * BLK], left_side=True, lower=True)
        updated = matrix - jnp.dot(column, solved, precision=lax.Precision.HIGHEST)
        matrix = jnp.where((row_block > target)[:, None], updated, matrix)
        matrix = matrix.at[target * BLK:(target + 1) * BLK].set(solved)
        solved_list.append(solved)
    stacked = jnp.concatenate(solved_list, 0)
    gram = jnp.dot(stacked.T, stacked, precision=lax.Precision.HIGHEST) * (1.0 / (STEPS * BLK))
    gram_part = gram.reshape(LR, N_ROW, BLK, LC, N_COL, BLK)
    finished = matrix[:FIN * BLK].reshape(FIN * BLK, LC, N_COL, BLK).transpose(0, 2, 1, 3)
    finished_columns = finished.reshape(LF, N_ROW, BLK, N_COL, N_ROW, CW)
    return (gram_part, finished_columns)
```

```python
import functools

import jax
import jax.numpy as jnp
from jax import lax
from jax.experimental import pallas as pl
from jax.experimental.pallas import tpu as pltpu
from jax.sharding import PartitionSpec as P


K = 30
STEPS = 2
LANES = 128
HIGHEST = lax.Precision.HIGHEST


def copy_block(_, source, target):
    target[...] = source[...]


def copy_into(_, source, __, target):
    target[...] = source[...]


def cost(flops, nbytes):
    return pl.CostEstimate(flops=int(flops), bytes_accessed=int(nbytes), transcendentals=0)


def pack(place, view, first, count):
    _, width, _, group, lanes = view.shape
    return pl.pallas_call(
        copy_block,
        grid_spec=pltpu.PrefetchScalarGridSpec(
            num_scalar_prefetch=1,
            grid=(count,),
            in_specs=[
                pl.BlockSpec((None, width, None, group, lanes), lambda f, at: (f + first, 0, at[0], 0, 0))
            ],
            out_specs=pl.BlockSpec((None, width, group, lanes), lambda f, at: (f, 0, 0, 0)),
        ),
        out_shape=jax.ShapeDtypeStruct((count, width, group, lanes), jnp.float32),
        cost_estimate=cost(0, 2 * 4 * count * width * group * lanes),
        name="pack",
    )(place, view)


def place_own(place, view, count, row_count):
    _, width, _, group, lanes = view.shape
    return pl.pallas_call(
        copy_block,
        grid_spec=pltpu.PrefetchScalarGridSpec(
            num_scalar_prefetch=1,
            grid=(count,),
            in_specs=[pl.BlockSpec((None, width, None, group, lanes), lambda f, at: (f, 0, at[0], 0, 0))],
            out_specs=pl.BlockSpec((None, None, width, group, lanes), lambda f, at: (f, at[0], 0, 0, 0)),
        ),
        out_shape=jax.ShapeDtypeStruct((count, row_count, width, group, lanes), jnp.float32),
        cost_estimate=cost(0, 2 * 4 * count * width * group * lanes),
        name="place_own",
    )(place, view)


def place_piece(place, piece, finished, first):
    count, width, group, lanes = piece.shape
    return pl.pallas_call(
        copy_into,
        grid_spec=pltpu.PrefetchScalarGridSpec(
            num_scalar_prefetch=1,
            grid=(count,),
            in_specs=[
                pl.BlockSpec((None, width, group, lanes), lambda f, at: (f, 0, 0, 0)),
                pl.BlockSpec(memory_space=pl.ANY),
            ],
            out_specs=pl.BlockSpec(
                (None, None, width, group, lanes), lambda f, at: (f + first, at[0], 0, 0, 0)
            ),
        ),
        out_shape=jax.ShapeDtypeStruct(finished.shape, jnp.float32),
        input_output_aliases={2: 0},
        cost_estimate=cost(0, 2 * 4 * piece.size),
        name="place_piece",
    )(place, piece, finished)


def solved_into(_, source, __, target):
    for part in range(target.shape[1]):
        target[:, part, :] = source[:, part * LANES : (part + 1) * LANES]


def place_solved(place, solved, finished, local, owners):
    _, _, width, group, lanes = finished.shape
    first = owners[0]
    return pl.pallas_call(
        solved_into,
        grid_spec=pltpu.PrefetchScalarGridSpec(
            num_scalar_prefetch=1,
            grid=(len(owners),),
            in_specs=[
                pl.BlockSpec((width, group * lanes), lambda s, at: (s, at[0])),
                pl.BlockSpec(memory_space=pl.ANY),
            ],
            out_specs=pl.BlockSpec(
                (None, None, width, group, lanes), lambda s, at: (local, s + first, 0, 0, 0)
            ),
        ),
        out_shape=jax.ShapeDtypeStruct(finished.shape, jnp.float32),
        input_output_aliases={2: 0},
        cost_estimate=cost(0, 2 * 4 * len(owners) * width * group * lanes),
        name="place_solved",
    )(place, solved, finished)


def solved_tile(inverse, source, block, stride, width):
    slabs = []
    for step in range(STEPS):
        halves = [
            source[step, pl.ds(block * (width // LANES) + half, width, stride=stride), :]
            for half in range(width // LANES)
        ]
        slabs.append(jnp.concatenate(halves, 1))
    return jnp.dot(
        inverse[...], jnp.concatenate(slabs, 0), precision=HIGHEST, preferred_element_type=jnp.float32
    )


def split_store(value, high, low):
    top = value.astype(jnp.bfloat16)
    high[...] = top
    low[...] = (value - top.astype(jnp.float32)).astype(jnp.bfloat16)


def solve_local_body(stride, width, inverse, source, solved, high, low):
    value = solved_tile(inverse, source, pl.program_id(0), stride, width)
    solved[...] = value
    split_store(value, high, low)


def solve_local(inverse, slabs, width):
    depth = STEPS * width
    stride = slabs.shape[1] // width
    columns = stride * LANES
    spec = pl.BlockSpec((depth, width), lambda j: (0, j))
    return pl.pallas_call(
        functools.partial(solve_local_body, stride, width),
        grid=(columns // width,),
        in_specs=[
            pl.BlockSpec((depth, depth), lambda j: (0, 0)),
            pl.BlockSpec(slabs.shape, lambda j: (0, 0, 0)),
        ],
        out_specs=[spec, spec, spec],
        out_shape=[
            jax.ShapeDtypeStruct((depth, columns), dtype)
            for dtype in (jnp.float32, jnp.bfloat16, jnp.bfloat16)
        ],
        cost_estimate=cost(12 * depth * depth * columns, 12 * depth * columns),
        name="solve_local",
    )(inverse, slabs)


def solve_panel_body(stride, width, inverse, source, high, low):
    value = solved_tile(inverse, source, pl.program_id(0), stride, width)
    split_store(value.T, high, low)


def solve_panel(inverse, slabs, width):
    depth = STEPS * width
    stride = slabs.shape[1] // width
    blocks = stride * LANES // width
    spec = pl.BlockSpec((None, width, depth), lambda j: (j, 0, 0))
    return pl.pallas_call(
        functools.partial(solve_panel_body, stride, width),
        grid=(blocks,),
        in_specs=[
            pl.BlockSpec((depth, depth), lambda j: (0, 0)),
            pl.BlockSpec(slabs.shape, lambda j: (0, 0, 0)),
        ],
        out_specs=[spec, spec],
        out_shape=[jax.ShapeDtypeStruct((blocks, width, depth), jnp.bfloat16)] * 2,
        cost_estimate=cost(12 * depth * depth * blocks * width, 8 * depth * blocks * width),
        name="solve_panel",
    )(inverse, slabs)


def gram_body(panels, scale, stride, width, *refs):
    panel_refs, (right_high, right_low, out) = refs[: 2 * panels], refs[2 * panels :]
    parts = width // LANES
    for panel in range(panels):
        left_high = panel_refs[2 * panel][...]
        left_low = panel_refs[2 * panel + 1][...]
        for block in range(stride // parts):
            at = slice(block * width, (block + 1) * width)
            high = right_high[:, at]
            total = jnp.dot(left_high, high, preferred_element_type=jnp.float32)
            total += jnp.dot(left_high, right_low[:, at], preferred_element_type=jnp.float32)
            total += jnp.dot(left_low, high, preferred_element_type=jnp.float32)
            total *= scale
            for part in range(parts):
                out[panel, pl.ds(block * parts + part, width, stride=stride), :] = total[
                    :, part * LANES : (part + 1) * LANES
                ]


def gram_product(panel_parts, right_high, right_low, scale):
    panels = len(panel_parts)
    blocks, width, depth = panel_parts[0][0].shape
    columns = right_high.shape[1]
    stride = columns // LANES
    left = pl.BlockSpec((None, width, depth), lambda j: (j, 0, 0))
    right = pl.BlockSpec((depth, columns), lambda j: (0, 0))
    return pl.pallas_call(
        functools.partial(gram_body, panels, scale, stride, width),
        grid=(blocks,),
        in_specs=[left] * (2 * panels) + [right] * 2,
        out_specs=pl.BlockSpec((None, panels, width * stride, LANES), lambda j: (j, 0, 0, 0)),
        out_shape=jax.ShapeDtypeStruct((blocks, panels, width * stride, LANES), jnp.float32),
        cost_estimate=cost(
            6 * depth * panels * blocks * width * columns, 4 * panels * blocks * width * columns
        ),
        name="gram",
    )(*[part for parts in panel_parts for part in parts], right_high, right_low)


def block_inverse(blocks):
    width = blocks[0][0].shape[0]
    eye = jnp.broadcast_to(jnp.eye(width, dtype=jnp.float32), (STEPS, width, width))
    diagonal = jnp.stack([jnp.tril(blocks[s][s]) for s in range(STEPS)])
    inner = lax.linalg.triangular_solve(diagonal, eye, left_side=True, lower=True)
    product = functools.partial(jnp.dot, precision=HIGHEST)
    rows = []
    for row in range(STEPS):
        line = []
        for column in range(STEPS):
            if column > row:
                line.append(jnp.zeros((width, width), jnp.float32))
            elif column == row:
                line.append(inner[row])
            else:
                total = sum(product(blocks[row][k], rows[k][column]) for k in range(column, row))
                line.append(-product(inner[row], total))
        rows.append(line)
    return jnp.concatenate([jnp.concatenate(line, 1) for line in rows], 0)


def window(working, factor_panel):
    row_count = lax.axis_size("row")
    col_count = lax.axis_size("col")
    row = lax.axis_index("row")
    col = lax.axis_index("col")
    blocks_rows, _, width, blocks_cols = working.shape[:4]
    columns = blocks_cols * width
    group = columns // row_count // LANES
    panels = col_count // row_count
    owners = [(K + step) % row_count for step in range(STEPS)]
    finished_count = (K + STEPS) // row_count
    local = finished_count - 1
    plain_rows = [index for index in range(row_count) if index not in owners]

    view = working.reshape(blocks_rows, width, row_count, group, LANES)
    slab = working.reshape(blocks_rows, width * columns // LANES, LANES)[local]

    def shifted(value, shift, senders):
        pairs = [(index, index ^ shift) for index in senders]
        return lax.ppermute(value, "row", pairs)

    part = width // col_count
    slices = lax.dynamic_slice_in_dim(factor_panel[:, local, 0], col * part, part, 1)
    heard = jnp.stack([slices] + [shifted(slices, shift, owners) for shift in range(1, row_count)])
    factor = jnp.stack(
        [lax.dynamic_index_in_dim(heard, row ^ owner, 0, False) for owner in owners]
    )
    size = 1
    while size < col_count:
        other = lax.ppermute(factor, "col", [(index, index ^ size) for index in range(col_count)])
        swap = (col & size) > 0
        factor = jnp.concatenate(
            [jnp.where(swap, other, factor), jnp.where(swap, factor, other)], 2
        )
        size *= 2
    inverse = block_inverse([[factor[s, t] for t in range(STEPS)] for s in range(STEPS)])

    def chain(step_sign):
        held, passed = slab, []
        for hop in range(1, row_count):
            pairs = []
            for owner in owners:
                at = owner + step_sign * hop
                if 0 <= at < row_count:
                    pairs.append((at - step_sign, at))
            if not pairs:
                break
            held = lax.ppermute(held, "row", pairs)
            passed.append(held)
        return passed

    down, up = chain(-1), chain(1)

    def block_row(owner):
        value = slab
        for hop, moved in enumerate(down, 1):
            value = jnp.where(row == owner - hop, moved, value)
        for hop, moved in enumerate(up, 1):
            value = jnp.where(row == owner + hop, moved, value)
        return value

    slabs = jnp.stack([block_row(owner) for owner in owners])

    at = [(row ^ shift).reshape(1) for shift in range(row_count)]
    finished = place_own(at[0], view, finished_count, row_count)
    packed = [pack(at[shift], view, local, 1) for shift in range(1, row_count)]
    last = [shifted(packed[shift - 1], shift, plain_rows) for shift in range(1, row_count)]
    ready = [pack(at[shift], view, 0, local) for shift in range(1, row_count)]
    through = down[-2] if len(down) > 1 else down[-1]
    ready, _ = lax.optimization_barrier((ready, through))
    rest = [shifted(ready[shift - 1], shift, range(row_count)) for shift in range(1, row_count)]

    both = ("row", "col")
    low_place = lax.rem(col, row_count)
    high_place = col // row_count

    def joined(value, holds, target):
        pairs = []
        for r in range(row_count):
            for c in range(col_count):
                if holds((c % row_count) ^ r):
                    pairs.append((r * col_count + c, r * col_count + target(c)))
        return lax.ppermute(value, both, pairs)

    held_bits = 0
    held = slabs
    bit = row_count // 2
    while bit > 1:
        moved = joined(held, lambda d, b=held_bits: d & ~b == 0, lambda c, b=bit: c ^ b)
        held = jnp.where((low_place ^ row) & bit > 0, moved, held)
        held_bits |= bit
        bit //= 2
    parts = [held]
    for shift in range(1, panels):
        parts.append(joined(held, lambda d: d & ~held_bits == 0, lambda c, s=shift: (c + s * row_count) % col_count))
    if row_count > 1:
        near = (low_place ^ row) & 1 > 0
        parts = [
            jnp.where(near, joined(value, lambda d: d & ~held_bits == 0, lambda c: c ^ 1), value)
            for value in parts
        ]
    panel_slabs = []
    for place in range(panels):
        value = parts[0]
        for shift in range(1, panels):
            value = jnp.where(lax.rem(high_place - place + panels, panels) == shift, parts[shift], value)
        panel_slabs.append(value)

    solved, right_high, right_low = solve_local(inverse, slabs, width)
    panel_parts = [solve_panel(inverse, value, width) for value in panel_slabs]
    gram = gram_product(panel_parts, right_high, right_low, 1.0 / (STEPS * width))

    for shift in range(1, row_count):
        finished = place_piece(at[shift], last[shift - 1], finished, local)
    finished = place_solved(at[0], solved, finished, local, owners)
    for shift in send_order(row_count):
        finished = place_piece(at[shift], rest[shift - 1], finished, 0)

    return (
        gram.reshape(working.shape),
        finished.reshape(finished_count, row_count, width, 1, 1, group * LANES),
    )


def send_order(row_count):
    return sorted(range(1, row_count), key=lambda shift: (shift == row_count - 1, -(shift & (row_count // 2)), shift))


def solution(mesh):
    return jax.shard_map(
        window,
        mesh=mesh,
        in_specs=(P(None, "row", None, None, "col", None), P(None, None, "row", None, None)),
        out_specs=(
            P(None, "row", None, None, "col", None),
            P(None, None, None, "col", "row", None),
        ),
        check_vma=False,
    )
```

```python
import functools

import jax
import jax.numpy as jnp
from jax import lax
from jax.experimental import pallas as pl
from jax.experimental.pallas import tpu as pltpu
from jax.sharding import PartitionSpec as P


K = 30
STEPS = 2
PARTS = 2
LANES = 128
HIGHEST = lax.Precision.HIGHEST


def copy_block(_, source, target):
    target[...] = source[...]


def copy_into(_, source, __, target):
    target[...] = source[...]


def cost(flops, nbytes):
    return pl.CostEstimate(flops=int(flops), bytes_accessed=int(nbytes), transcendentals=0)


def pack(place, view, first, count):
    _, width, _, group, lanes = view.shape
    return pl.pallas_call(
        copy_block,
        grid_spec=pltpu.PrefetchScalarGridSpec(
            num_scalar_prefetch=1,
            grid=(count,),
            in_specs=[
                pl.BlockSpec((None, width, None, group, lanes), lambda f, at: (f + first, 0, at[0], 0, 0))
            ],
            out_specs=pl.BlockSpec((None, width, group, lanes), lambda f, at: (f, 0, 0, 0)),
        ),
        out_shape=jax.ShapeDtypeStruct((count, width, group, lanes), jnp.float32),
        cost_estimate=cost(0, 2 * 4 * count * width * group * lanes),
        name="pack",
    )(place, view)


def place_own(place, view, count, row_count):
    _, width, _, group, lanes = view.shape
    return pl.pallas_call(
        copy_block,
        grid_spec=pltpu.PrefetchScalarGridSpec(
            num_scalar_prefetch=1,
            grid=(count,),
            in_specs=[pl.BlockSpec((None, width, None, group, lanes), lambda f, at: (f, 0, at[0], 0, 0))],
            out_specs=pl.BlockSpec((None, None, width, group, lanes), lambda f, at: (f, at[0], 0, 0, 0)),
        ),
        out_shape=jax.ShapeDtypeStruct((count, row_count, width, group, lanes), jnp.float32),
        cost_estimate=cost(0, 2 * 4 * count * width * group * lanes),
        name="place_own",
    )(place, view)


def place_piece(place, piece, finished, first):
    count, width, group, lanes = piece.shape
    return pl.pallas_call(
        copy_into,
        grid_spec=pltpu.PrefetchScalarGridSpec(
            num_scalar_prefetch=1,
            grid=(count,),
            in_specs=[
                pl.BlockSpec((None, width, group, lanes), lambda f, at: (f, 0, 0, 0)),
                pl.BlockSpec(memory_space=pl.ANY),
            ],
            out_specs=pl.BlockSpec(
                (None, None, width, group, lanes), lambda f, at: (f + first, at[0], 0, 0, 0)
            ),
        ),
        out_shape=jax.ShapeDtypeStruct(finished.shape, jnp.float32),
        input_output_aliases={2: 0},
        cost_estimate=cost(0, 2 * 4 * piece.size),
        name="place_piece",
    )(place, piece, finished)


def either_into(at, one, other, _, target):
    @pl.when(at[1] > 0)
    def _():
        target[...] = one[...]

    @pl.when(at[1] == 0)
    def _():
        target[...] = other[...]


def place_either(place, one, other, finished, first):
    count, width, group, lanes = one.shape
    return pl.pallas_call(
        either_into,
        grid_spec=pltpu.PrefetchScalarGridSpec(
            num_scalar_prefetch=1,
            grid=(count,),
            in_specs=[
                pl.BlockSpec((None, width, group, lanes), lambda f, at: (f * at[1], 0, 0, 0)),
                pl.BlockSpec((None, width, group, lanes), lambda f, at: (f * (1 - at[1]), 0, 0, 0)),
                pl.BlockSpec(memory_space=pl.ANY),
            ],
            out_specs=pl.BlockSpec(
                (None, None, width, group, lanes), lambda f, at: (f + first, at[0], 0, 0, 0)
            ),
        ),
        out_shape=jax.ShapeDtypeStruct(finished.shape, jnp.float32),
        input_output_aliases={3: 0},
        cost_estimate=cost(0, 2 * 4 * one.size),
        name="place_either",
    )(place, one, other, finished)


def solved_into(_, source, __, target):
    for part in range(target.shape[1]):
        target[:, part, :] = source[:, part * LANES : (part + 1) * LANES]


def place_solved(place, solved, finished, local, owners):
    _, _, width, group, lanes = finished.shape
    first = owners[0]
    return pl.pallas_call(
        solved_into,
        grid_spec=pltpu.PrefetchScalarGridSpec(
            num_scalar_prefetch=1,
            grid=(len(owners),),
            in_specs=[
                pl.BlockSpec((width, group * lanes), lambda s, at: (s, at[0])),
                pl.BlockSpec(memory_space=pl.ANY),
            ],
            out_specs=pl.BlockSpec(
                (None, None, width, group, lanes), lambda s, at: (local, s + first, 0, 0, 0)
            ),
        ),
        out_shape=jax.ShapeDtypeStruct(finished.shape, jnp.float32),
        input_output_aliases={2: 0},
        cost_estimate=cost(0, 2 * 4 * len(owners) * width * group * lanes),
        name="place_solved",
    )(place, solved, finished)


def solved_tile(inverse, source, block, stride, width):
    slabs = []
    for step in range(STEPS):
        halves = [
            source[step, pl.ds(block * (width // LANES) + half, width, stride=stride), :]
            for half in range(width // LANES)
        ]
        slabs.append(jnp.concatenate(halves, 1))
    return jnp.dot(
        inverse[...], jnp.concatenate(slabs, 0), precision=HIGHEST, preferred_element_type=jnp.float32
    )


def split_store(value, high, low):
    top = value.astype(jnp.bfloat16)
    high[...] = top
    low[...] = (value - top.astype(jnp.float32)).astype(jnp.bfloat16)


def solve_local_body(stride, width, inverse, source, solved, high, low):
    value = solved_tile(inverse, source, pl.program_id(0), stride, width)
    solved[...] = value
    split_store(value, high, low)


def solve_local(inverse, slabs, width):
    depth = STEPS * width
    stride = slabs.shape[1] // width
    columns = stride * LANES
    spec = pl.BlockSpec((depth, width), lambda j: (0, j))
    return pl.pallas_call(
        functools.partial(solve_local_body, stride, width),
        grid=(columns // width,),
        in_specs=[
            pl.BlockSpec((depth, depth), lambda j: (0, 0)),
            pl.BlockSpec(slabs.shape, lambda j: (0, 0, 0)),
        ],
        out_specs=[spec, spec, spec],
        out_shape=[
            jax.ShapeDtypeStruct((depth, columns), dtype)
            for dtype in (jnp.float32, jnp.bfloat16, jnp.bfloat16)
        ],
        cost_estimate=cost(12 * depth * depth * columns, 12 * depth * columns),
        name="solve_local",
    )(inverse, slabs)


def solve_panel_body(stride, width, inverse, source, high, low):
    value = solved_tile(inverse, source, pl.program_id(0), stride, width)
    split_store(value.T, high, low)


def solve_panel(inverse, slabs, width):
    depth = STEPS * width
    stride = slabs.shape[1] // width
    blocks = stride * LANES // width
    spec = pl.BlockSpec((None, width, depth), lambda j: (j, 0, 0))
    return pl.pallas_call(
        functools.partial(solve_panel_body, stride, width),
        grid=(blocks,),
        in_specs=[
            pl.BlockSpec((depth, depth), lambda j: (0, 0)),
            pl.BlockSpec(slabs.shape, lambda j: (0, 0, 0)),
        ],
        out_specs=[spec, spec],
        out_shape=[jax.ShapeDtypeStruct((blocks, width, depth), jnp.bfloat16)] * 2,
        cost_estimate=cost(12 * depth * depth * blocks * width, 8 * depth * blocks * width),
        name="solve_panel",
    )(inverse, slabs)


def gram_body(panels, scale, stride, width, *refs):
    panel_refs, (right_high, right_low, out) = refs[: 2 * panels], refs[2 * panels :]
    parts = width // LANES
    for panel in range(panels):
        left_high = panel_refs[2 * panel][...]
        left_low = panel_refs[2 * panel + 1][...]
        for block in range(stride // parts):
            at = slice(block * width, (block + 1) * width)
            high = right_high[:, at]
            total = jnp.dot(left_high, high, preferred_element_type=jnp.float32)
            total += jnp.dot(left_high, right_low[:, at], preferred_element_type=jnp.float32)
            total += jnp.dot(left_low, high, preferred_element_type=jnp.float32)
            total *= scale
            for part in range(parts):
                out[panel, pl.ds(block * parts + part, width, stride=stride), :] = total[
                    :, part * LANES : (part + 1) * LANES
                ]


def gram_product(panel_parts, right_high, right_low, scale):
    panels = len(panel_parts)
    blocks, width, depth = panel_parts[0][0].shape
    columns = right_high.shape[1]
    stride = columns // LANES
    left = pl.BlockSpec((None, width, depth), lambda j: (j, 0, 0))
    right = pl.BlockSpec((depth, columns), lambda j: (0, 0))
    return pl.pallas_call(
        functools.partial(gram_body, panels, scale, stride, width),
        grid=(blocks,),
        in_specs=[left] * (2 * panels) + [right] * 2,
        out_specs=pl.BlockSpec((None, panels, width * stride, LANES), lambda j: (j, 0, 0, 0)),
        out_shape=jax.ShapeDtypeStruct((blocks, panels, width * stride, LANES), jnp.float32),
        cost_estimate=cost(
            6 * depth * panels * blocks * width * columns, 4 * panels * blocks * width * columns
        ),
        name="gram",
    )(*[part for parts in panel_parts for part in parts], right_high, right_low)


def block_inverse(blocks):
    width = blocks[0][0].shape[0]
    eye = jnp.broadcast_to(jnp.eye(width, dtype=jnp.float32), (STEPS, width, width))
    diagonal = jnp.stack([jnp.tril(blocks[s][s]) for s in range(STEPS)])
    inner = lax.linalg.triangular_solve(diagonal, eye, left_side=True, lower=True)
    product = functools.partial(jnp.dot, precision=HIGHEST)
    rows = []
    for row in range(STEPS):
        line = []
        for column in range(STEPS):
            if column > row:
                line.append(jnp.zeros((width, width), jnp.float32))
            elif column == row:
                line.append(inner[row])
            else:
                total = sum(product(blocks[row][k], rows[k][column]) for k in range(column, row))
                line.append(-product(inner[row], total))
        rows.append(line)
    return jnp.concatenate([jnp.concatenate(line, 1) for line in rows], 0)


def window(working, factor_panel):
    row_count = lax.axis_size("row")
    col_count = lax.axis_size("col")
    row = lax.axis_index("row")
    col = lax.axis_index("col")
    blocks_rows, _, width, blocks_cols = working.shape[:4]
    columns = blocks_cols * width
    group = columns // row_count // LANES
    panels = col_count // row_count
    owners = [(K + step) % row_count for step in range(STEPS)]
    finished_count = (K + STEPS) // row_count
    local = finished_count - 1
    plain_rows = [index for index in range(row_count) if index not in owners]

    view = working.reshape(blocks_rows, width, row_count, group, LANES)
    slab_rows = width * columns // LANES // PARTS
    slab_parts = working.reshape(blocks_rows, PARTS, slab_rows, LANES)
    slab = [slab_parts[local, part] for part in range(PARTS)]

    def shifted(value, shift, senders):
        pairs = [(index, index ^ shift) for index in senders]
        return lax.ppermute(value, "row", pairs)

    def chain(step_sign, part):
        held, passed = slab[part], []
        for hop in range(1, row_count):
            pairs = []
            for owner in owners:
                at = owner + step_sign * hop
                if 0 <= at < row_count:
                    pairs.append((at - step_sign, at))
            if not pairs:
                break
            held = lax.ppermute(held, "row", pairs)
            passed.append(held)
        return passed

    down = [chain(-1, part) for part in range(PARTS)]
    up = [chain(1, part) for part in range(PARTS)]

    part = width // col_count
    slices = lax.dynamic_slice_in_dim(factor_panel[:, local, 0], col * part, part, 1)
    heard = [slices] + [shifted(slices, shift, owners) for shift in range(1, row_count)]
    heard, _ = lax.optimization_barrier((heard, down[-1][0]))
    heard = jnp.stack(heard)
    factor = jnp.stack(
        [lax.dynamic_index_in_dim(heard, row ^ owner, 0, False) for owner in owners]
    )
    size = 1
    while size < col_count:
        other = lax.ppermute(factor, "col", [(index, index ^ size) for index in range(col_count)])
        swap = (col & size) > 0
        factor = jnp.concatenate(
            [jnp.where(swap, other, factor), jnp.where(swap, factor, other)], 2
        )
        size *= 2
    inverse = block_inverse([[factor[s, t] for t in range(STEPS)] for s in range(STEPS)])

    def block_row(owner, part):
        value = slab[part]
        for hop, moved in enumerate(down[part], 1):
            value = jnp.where(row == owner - hop, moved, value)
        for hop, moved in enumerate(up[part], 1):
            value = jnp.where(row == owner + hop, moved, value)
        return value

    slabs = jnp.stack(
        [jnp.concatenate([block_row(owner, part) for part in range(PARTS)], 0) for owner in owners]
    )

    at = [(row ^ shift).reshape(1) for shift in range(row_count)]
    finished = place_own(at[0], view, finished_count, row_count)
    packed = [pack(at[shift], view, local, 1) for shift in range(1, row_count)]
    last = [shifted(packed[shift - 1], shift, plain_rows) for shift in range(1, row_count)]
    ready = {
        (shift, first): pack(at[shift], view, first, count)
        for shift in range(1, row_count)
        for first, count in pieces(shift, row_count, local)
    }
    middle = row_count // 2
    inner = [middle - 1, middle]
    outer = [index for index in range(row_count) if index not in inner]
    rest = {}
    for (shift, first), value in ready.items():
        if shift == middle:
            rest[shift, first] = (shifted(value, shift, inner), shifted(value, shift, outer))
        else:
            rest[shift, first] = (shifted(value, shift, range(row_count)),)

    both = ("row", "col")
    low_place = lax.rem(col, row_count)
    high_place = col // row_count

    def joined(value, holds, target):
        pairs = []
        for r in range(row_count):
            for c in range(col_count):
                if holds((c % row_count) ^ r):
                    pairs.append((r * col_count + c, r * col_count + target(c)))
        return lax.ppermute(value, both, pairs)

    held_bits = 0
    held = slabs
    bit = row_count // 2
    while bit > 1:
        moved = joined(held, lambda d, b=held_bits: d & ~b == 0, lambda c, b=bit: c ^ b)
        held = jnp.where((low_place ^ row) & bit > 0, moved, held)
        held_bits |= bit
        bit //= 2
    parts = [held]
    for shift in range(1, panels):
        parts.append(joined(held, lambda d: d & ~held_bits == 0, lambda c, s=shift: (c + s * row_count) % col_count))
    if row_count > 1:
        near = (low_place ^ row) & 1 > 0
        parts = [
            jnp.where(near, joined(value, lambda d: d & ~held_bits == 0, lambda c: c ^ 1), value)
            for value in parts
        ]
    panel_slabs = []
    for place in range(panels):
        value = parts[0]
        for shift in range(1, panels):
            value = jnp.where(lax.rem(high_place - place + panels, panels) == shift, parts[shift], value)
        panel_slabs.append(value)

    solved, right_high, right_low = solve_local(inverse, slabs, width)
    panel_parts = [solve_panel(inverse, value, width) for value in panel_slabs]
    gram = gram_product(panel_parts, right_high, right_low, 1.0 / (STEPS * width))

    for shift in range(1, row_count):
        finished = place_piece(at[shift], last[shift - 1], finished, local)
    finished = place_solved(at[0], solved, finished, local, owners)
    from_inner = ((row ^ middle) == inner[0]) | ((row ^ middle) == inner[1])
    for shift in send_order(row_count):
        for first, _ in pieces(shift, row_count, local):
            if shift == middle:
                finished = place_either(
                    jnp.concatenate([at[shift], from_inner.astype(jnp.int32).reshape(1)]),
                    *rest[shift, first],
                    finished,
                    first,
                )
            else:
                finished = place_piece(at[shift], *rest[shift, first], finished, first)

    return (
        gram.reshape(working.shape),
        finished.reshape(finished_count, row_count, width, 1, 1, group * LANES),
    )


def send_order(row_count):
    return sorted(range(1, row_count), key=lambda shift: (shift == row_count - 1, -(shift & (row_count // 2)), shift))


def pieces(shift, row_count, count):
    small = max(count // 4, 1)
    if shift == row_count - 1 and count > small:
        return [(0, count - small), (count - small, small)]
    return [(0, count)]


def solution(mesh):
    return jax.shard_map(
        window,
        mesh=mesh,
        in_specs=(P(None, "row", None, None, "col", None), P(None, None, "row", None, None)),
        out_specs=(
            P(None, "row", None, None, "col", None),
            P(None, None, None, "col", "row", None),
        ),
        check_vma=False,
    )
```

```python
import functools

import jax
import jax.numpy as jnp
from jax import lax
from jax.experimental import pallas as pl
from jax.experimental.pallas import tpu as pltpu
from jax.sharding import PartitionSpec as P


K = 30
STEPS = 2
PARTS = 2
LANES = 128
HIGHEST = lax.Precision.HIGHEST


def copy_block(_, source, target):
    target[...] = source[...]


def copy_into(_, source, __, target):
    target[...] = source[...]


def cost(flops, nbytes):
    return pl.CostEstimate(flops=int(flops), bytes_accessed=int(nbytes), transcendentals=0)


def pack(place, view, first, count):
    _, width, _, group, lanes = view.shape
    return pl.pallas_call(
        copy_block,
        grid_spec=pltpu.PrefetchScalarGridSpec(
            num_scalar_prefetch=1,
            grid=(count,),
            in_specs=[
                pl.BlockSpec((None, width, None, group, lanes), lambda f, at: (f + first, 0, at[0], 0, 0))
            ],
            out_specs=pl.BlockSpec((None, width, group, lanes), lambda f, at: (f, 0, 0, 0)),
        ),
        out_shape=jax.ShapeDtypeStruct((count, width, group, lanes), jnp.float32),
        cost_estimate=cost(0, 2 * 4 * count * width * group * lanes),
        name="pack",
    )(place, view)


def place_own(place, view, count, row_count):
    _, width, _, group, lanes = view.shape
    return pl.pallas_call(
        copy_block,
        grid_spec=pltpu.PrefetchScalarGridSpec(
            num_scalar_prefetch=1,
            grid=(count,),
            in_specs=[pl.BlockSpec((None, width, None, group, lanes), lambda f, at: (f, 0, at[0], 0, 0))],
            out_specs=pl.BlockSpec((None, None, width, group, lanes), lambda f, at: (f, at[0], 0, 0, 0)),
        ),
        out_shape=jax.ShapeDtypeStruct((count, row_count, width, group, lanes), jnp.float32),
        cost_estimate=cost(0, 2 * 4 * count * width * group * lanes),
        name="place_own",
    )(place, view)


def place_piece(place, piece, finished, first):
    count, width, group, lanes = piece.shape
    return pl.pallas_call(
        copy_into,
        grid_spec=pltpu.PrefetchScalarGridSpec(
            num_scalar_prefetch=1,
            grid=(count,),
            in_specs=[
                pl.BlockSpec((None, width, group, lanes), lambda f, at: (f, 0, 0, 0)),
                pl.BlockSpec(memory_space=pl.ANY),
            ],
            out_specs=pl.BlockSpec(
                (None, None, width, group, lanes), lambda f, at: (f + first, at[0], 0, 0, 0)
            ),
        ),
        out_shape=jax.ShapeDtypeStruct(finished.shape, jnp.float32),
        input_output_aliases={2: 0},
        cost_estimate=cost(0, 2 * 4 * piece.size),
        name="place_piece",
    )(place, piece, finished)


def either_into(at, one, other, _, target):
    @pl.when(at[1] > 0)
    def _():
        target[...] = one[...]

    @pl.when(at[1] == 0)
    def _():
        target[...] = other[...]


def place_either(place, one, other, finished, first):
    count, width, group, lanes = one.shape
    return pl.pallas_call(
        either_into,
        grid_spec=pltpu.PrefetchScalarGridSpec(
            num_scalar_prefetch=1,
            grid=(count,),
            in_specs=[
                pl.BlockSpec((None, width, group, lanes), lambda f, at: (f * at[1], 0, 0, 0)),
                pl.BlockSpec((None, width, group, lanes), lambda f, at: (f * (1 - at[1]), 0, 0, 0)),
                pl.BlockSpec(memory_space=pl.ANY),
            ],
            out_specs=pl.BlockSpec(
                (None, None, width, group, lanes), lambda f, at: (f + first, at[0], 0, 0, 0)
            ),
        ),
        out_shape=jax.ShapeDtypeStruct(finished.shape, jnp.float32),
        input_output_aliases={3: 0},
        cost_estimate=cost(0, 2 * 4 * one.size),
        name="place_either",
    )(place, one, other, finished)


def solved_into(_, source, __, target):
    for part in range(target.shape[1]):
        target[:, part, :] = source[:, part * LANES : (part + 1) * LANES]


def place_solved(place, solved, finished, local, owners):
    _, _, width, group, lanes = finished.shape
    first = owners[0]
    return pl.pallas_call(
        solved_into,
        grid_spec=pltpu.PrefetchScalarGridSpec(
            num_scalar_prefetch=1,
            grid=(len(owners),),
            in_specs=[
                pl.BlockSpec((width, group * lanes), lambda s, at: (s, at[0])),
                pl.BlockSpec(memory_space=pl.ANY),
            ],
            out_specs=pl.BlockSpec(
                (None, None, width, group, lanes), lambda s, at: (local, s + first, 0, 0, 0)
            ),
        ),
        out_shape=jax.ShapeDtypeStruct(finished.shape, jnp.float32),
        input_output_aliases={2: 0},
        cost_estimate=cost(0, 2 * 4 * len(owners) * width * group * lanes),
        name="place_solved",
    )(place, solved, finished)


def solved_tile(inverse, source, block, stride, width):
    slabs = []
    for step in range(STEPS):
        halves = [
            source[step, pl.ds(block * (width // LANES) + half, width, stride=stride), :]
            for half in range(width // LANES)
        ]
        slabs.append(jnp.concatenate(halves, 1))
    return jnp.dot(
        inverse[...], jnp.concatenate(slabs, 0), precision=HIGHEST, preferred_element_type=jnp.float32
    )


def split_store(value, high, low):
    top = value.astype(jnp.bfloat16)
    high[...] = top
    low[...] = (value - top.astype(jnp.float32)).astype(jnp.bfloat16)


def solve_local_body(stride, width, inverse, source, solved, high, low):
    value = solved_tile(inverse, source, pl.program_id(0), stride, width)
    solved[...] = value
    split_store(value, high, low)


def solve_local(inverse, slabs, width):
    depth = STEPS * width
    stride = slabs.shape[1] // width
    columns = stride * LANES
    spec = pl.BlockSpec((depth, width), lambda j: (0, j))
    return pl.pallas_call(
        functools.partial(solve_local_body, stride, width),
        grid=(columns // width,),
        in_specs=[
            pl.BlockSpec((depth, depth), lambda j: (0, 0)),
            pl.BlockSpec(slabs.shape, lambda j: (0, 0, 0)),
        ],
        out_specs=[spec, spec, spec],
        out_shape=[
            jax.ShapeDtypeStruct((depth, columns), dtype)
            for dtype in (jnp.float32, jnp.bfloat16, jnp.bfloat16)
        ],
        cost_estimate=cost(12 * depth * depth * columns, 12 * depth * columns),
        name="solve_local",
    )(inverse, slabs)


def solve_panel_body(stride, width, inverse, source, high, low):
    value = solved_tile(inverse, source, pl.program_id(0), stride, width)
    split_store(value.T, high, low)


def solve_panel(inverse, slabs, width):
    depth = STEPS * width
    stride = slabs.shape[1] // width
    blocks = stride * LANES // width
    spec = pl.BlockSpec((None, width, depth), lambda j: (j, 0, 0))
    return pl.pallas_call(
        functools.partial(solve_panel_body, stride, width),
        grid=(blocks,),
        in_specs=[
            pl.BlockSpec((depth, depth), lambda j: (0, 0)),
            pl.BlockSpec(slabs.shape, lambda j: (0, 0, 0)),
        ],
        out_specs=[spec, spec],
        out_shape=[jax.ShapeDtypeStruct((blocks, width, depth), jnp.bfloat16)] * 2,
        cost_estimate=cost(12 * depth * depth * blocks * width, 8 * depth * blocks * width),
        name="solve_panel",
    )(inverse, slabs)


def gram_body(panels, scale, stride, width, *refs):
    panel_refs, (right_high, right_low, out) = refs[: 2 * panels], refs[2 * panels :]
    parts = width // LANES
    for panel in range(panels):
        left_high = panel_refs[2 * panel][...]
        left_low = panel_refs[2 * panel + 1][...]
        for block in range(stride // parts):
            at = slice(block * width, (block + 1) * width)
            high = right_high[:, at]
            total = jnp.dot(left_high, high, preferred_element_type=jnp.float32)
            total += jnp.dot(left_high, right_low[:, at], preferred_element_type=jnp.float32)
            total += jnp.dot(left_low, high, preferred_element_type=jnp.float32)
            total *= scale
            for part in range(parts):
                out[panel, pl.ds(block * parts + part, width, stride=stride), :] = total[
                    :, part * LANES : (part + 1) * LANES
                ]


def gram_product(panel_parts, right_high, right_low, scale):
    panels = len(panel_parts)
    blocks, width, depth = panel_parts[0][0].shape
    columns = right_high.shape[1]
    stride = columns // LANES
    left = pl.BlockSpec((None, width, depth), lambda j: (j, 0, 0))
    right = pl.BlockSpec((depth, columns), lambda j: (0, 0))
    return pl.pallas_call(
        functools.partial(gram_body, panels, scale, stride, width),
        grid=(blocks,),
        in_specs=[left] * (2 * panels) + [right] * 2,
        out_specs=pl.BlockSpec((None, panels, width * stride, LANES), lambda j: (j, 0, 0, 0)),
        out_shape=jax.ShapeDtypeStruct((blocks, panels, width * stride, LANES), jnp.float32),
        cost_estimate=cost(
            6 * depth * panels * blocks * width * columns, 4 * panels * blocks * width * columns
        ),
        name="gram",
    )(*[part for parts in panel_parts for part in parts], right_high, right_low)


def block_inverse(blocks):
    width = blocks[0][0].shape[0]
    eye = jnp.broadcast_to(jnp.eye(width, dtype=jnp.float32), (STEPS, width, width))
    diagonal = jnp.stack([jnp.tril(blocks[s][s]) for s in range(STEPS)])
    inner = lax.linalg.triangular_solve(diagonal, eye, left_side=True, lower=True)
    product = functools.partial(jnp.dot, precision=HIGHEST)
    rows = []
    for row in range(STEPS):
        line = []
        for column in range(STEPS):
            if column > row:
                line.append(jnp.zeros((width, width), jnp.float32))
            elif column == row:
                line.append(inner[row])
            else:
                total = sum(product(blocks[row][k], rows[k][column]) for k in range(column, row))
                line.append(-product(inner[row], total))
        rows.append(line)
    return jnp.concatenate([jnp.concatenate(line, 1) for line in rows], 0)


def window(working, factor_panel):
    row_count = lax.axis_size("row")
    col_count = lax.axis_size("col")
    row = lax.axis_index("row")
    col = lax.axis_index("col")
    blocks_rows, _, width, blocks_cols = working.shape[:4]
    columns = blocks_cols * width
    group = columns // row_count // LANES
    panels = col_count // row_count
    owners = [(K + step) % row_count for step in range(STEPS)]
    finished_count = (K + STEPS) // row_count
    local = finished_count - 1
    plain_rows = [index for index in range(row_count) if index not in owners]

    view = working.reshape(blocks_rows, width, row_count, group, LANES)
    whole_slab = working.reshape(blocks_rows, width * columns // LANES, LANES)
    cut = whole_slab.shape[1] * 3 // 8
    slab = [whole_slab[local, :cut], whole_slab[local, cut:]]

    def shifted(value, shift, senders):
        pairs = [(index, index ^ shift) for index in senders]
        return lax.ppermute(value, "row", pairs)

    def chain(step_sign, part):
        held, passed = slab[part], []
        for hop in range(1, row_count):
            pairs = []
            for owner in owners:
                at = owner + step_sign * hop
                if 0 <= at < row_count:
                    pairs.append((at - step_sign, at))
            if not pairs:
                break
            held = lax.ppermute(held, "row", pairs)
            passed.append(held)
        return passed

    down = [chain(-1, part) for part in range(PARTS)]
    up = [chain(1, part) for part in range(PARTS)]

    part = width // col_count
    slices = lax.dynamic_slice_in_dim(factor_panel[:, local, 0], col * part, part, 1)
    heard = []
    for turn in range(1, STEPS):
        pairs = [(owners[s], owners[(s + turn) % STEPS]) for s in range(STEPS)]
        heard.append(lax.ppermute(slices, "row", pairs))
    factor = []
    for step in range(STEPS):
        value = slices
        for turn in range(1, STEPS):
            value = jnp.where(row == owners[(step + turn) % STEPS], heard[turn - 1], value)
        factor += [value[t] for t in range(step + 1)]
    factor = jnp.stack(factor)
    for hop in range(1, row_count):
        pairs, ends = [], (min(owners) - hop, max(owners) + hop)
        if ends[0] >= 0:
            pairs.append((ends[0] + 1, ends[0]))
        if ends[1] < row_count:
            pairs.append((ends[1] - 1, ends[1]))
        if not pairs:
            break
        moved = lax.ppermute(factor, "row", pairs)
        factor = jnp.where((row == ends[0]) | (row == ends[1]), moved, factor)
    size = 1
    while size < col_count:
        other = lax.ppermute(factor, "col", [(index, index ^ size) for index in range(col_count)])
        swap = (col & size) > 0
        factor = jnp.concatenate([jnp.where(swap, other, factor), jnp.where(swap, factor, other)], 1)
        size *= 2
    inverse = block_inverse(
        [[factor[s * (s + 1) // 2 + t] for t in range(s + 1)] for s in range(STEPS)]
    )

    def block_row(owner, part):
        value = slab[part]
        for hop, moved in enumerate(down[part], 1):
            value = jnp.where(row == owner - hop, moved, value)
        for hop, moved in enumerate(up[part], 1):
            value = jnp.where(row == owner + hop, moved, value)
        return value

    slabs = jnp.stack(
        [jnp.concatenate([block_row(owner, part) for part in range(PARTS)], 0) for owner in owners]
    )

    at = [(row ^ shift).reshape(1) for shift in range(row_count)]
    finished = place_own(at[0], view, finished_count, row_count)
    packed = [pack(at[shift], view, local, 1) for shift in range(1, row_count)]
    last = [shifted(packed[shift - 1], shift, plain_rows) for shift in range(1, row_count)]
    ready = {
        (shift, first): pack(at[shift], view, first, count)
        for shift in range(1, row_count)
        for first, count in pieces(shift, row_count, local)
    }
    middle = row_count // 2
    inner = [middle - 1, middle]
    outer = [index for index in range(row_count) if index not in inner]
    rest = {}
    for (shift, first), value in ready.items():
        if shift == middle:
            rest[shift, first] = (shifted(value, shift, inner), shifted(value, shift, outer))
        else:
            rest[shift, first] = (shifted(value, shift, range(row_count)),)

    both = ("row", "col")
    low_place = lax.rem(col, row_count)
    high_place = col // row_count

    def joined(value, holds, target):
        pairs = []
        for r in range(row_count):
            for c in range(col_count):
                if holds((c % row_count) ^ r):
                    pairs.append((r * col_count + c, r * col_count + target(c)))
        return lax.ppermute(value, both, pairs)

    held_bits = 0
    held = slabs
    bit = row_count // 2
    while bit > 1:
        moved = joined(held, lambda d, b=held_bits: d & ~b == 0, lambda c, b=bit: c ^ b)
        held = jnp.where((low_place ^ row) & bit > 0, moved, held)
        held_bits |= bit
        bit //= 2
    parts = [held]
    for shift in range(1, panels):
        parts.append(joined(held, lambda d: d & ~held_bits == 0, lambda c, s=shift: (c + s * row_count) % col_count))
    if row_count > 1:
        near = (low_place ^ row) & 1 > 0
        parts = [
            jnp.where(near, joined(value, lambda d: d & ~held_bits == 0, lambda c: c ^ 1), value)
            for value in parts
        ]
    panel_slabs = []
    for place in range(panels):
        value = parts[0]
        for shift in range(1, panels):
            value = jnp.where(lax.rem(high_place - place + panels, panels) == shift, parts[shift], value)
        panel_slabs.append(value)

    solved, right_high, right_low = solve_local(inverse, slabs, width)
    panel_parts = [solve_panel(inverse, value, width) for value in panel_slabs]
    gram = gram_product(panel_parts, right_high, right_low, 1.0 / (STEPS * width))

    for shift in range(1, row_count):
        finished = place_piece(at[shift], last[shift - 1], finished, local)
    finished = place_solved(at[0], solved, finished, local, owners)
    from_inner = ((row ^ middle) == inner[0]) | ((row ^ middle) == inner[1])
    for shift in send_order(row_count):
        for first, _ in pieces(shift, row_count, local):
            if shift == middle:
                finished = place_either(
                    jnp.concatenate([at[shift], from_inner.astype(jnp.int32).reshape(1)]),
                    *rest[shift, first],
                    finished,
                    first,
                )
            else:
                finished = place_piece(at[shift], *rest[shift, first], finished, first)

    return (
        gram.reshape(working.shape),
        finished.reshape(finished_count, row_count, width, 1, 1, group * LANES),
    )


def send_order(row_count):
    return sorted(range(1, row_count), key=lambda shift: (shift == row_count - 1, -(shift & (row_count // 2)), shift))


def pieces(shift, row_count, count):
    small = max(count // 4, 1)
    if shift == row_count - 1 and count > small:
        return [(0, count - small), (count - small, small)]
    return [(0, count)]


def solution(mesh):
    return jax.shard_map(
        window,
        mesh=mesh,
        in_specs=(P(None, "row", None, None, "col", None), P(None, None, "row", None, None)),
        out_specs=(
            P(None, "row", None, None, "col", None),
            P(None, None, None, "col", "row", None),
        ),
        check_vma=False,
    )
```
